32 devices in a mesh: tm: 4 (over y, core), space: 8 (over z, x).
Axes of the slice: x: 2, y: 2, z: 4, core: 2. Of those that a mesh axis runs over, the one named last changes fastest.
Arguments:
- state: bfloat16 [4, 4096, 137], P('tm', 'space'), may hold values from -6 to 6
- obs_start: int32 [16384], P(('tm', 'space')), may hold values from 0 to 4095, as said below
- foot_weight: bfloat16 [16384, 8], P(('tm', 'space')), may hold values from 0.019897461 to 0.29882812
- obs_slot: int32 [16384], P(('tm', 'space')), may hold values from 0 to 2
- obs_frac: float32 [16384], P(('tm', 'space')), may hold values from 0 to 1
- live_count: int32 [4, 8], P('tm', 'space'), may hold values from 64 to 512
- obs_values: float32 [16384, 128], P(('tm', 'space')), may hold values from -6 to 6
- jacobian: bfloat16 [137, 128], replicated, may hold values from -0.5 to 0.5
- inv_var: float32 [128], replicated, may hold values from 0.25 to 4
Outputs:
- departures: float32 [16384, 128], P(('tm', 'space'))
- adjoint: float32 [4, 4096, 137], P('tm', 'space')
The draws below stay inside these ranges and needn't reach their ends.
Inputs may be any that keep to these rules, and one draw needn't show every extreme that they name: `obs_start`: on the devices of space index s, every observation's footprint columns lie within 256 columns of tile s, that is within s * 512 - 256 .. (s + 1) * 512 + 255 taken modulo 4096. `live_count`: rows at or beyond a device's count are padding.
All inputs are finite; a program needn't handle non-finite values.
Results may differ from the reference program's by a relative error of at most 0.008.
Values may be sent and summed in bfloat16 or wider, within the bound.
A program may use at most 64 MiB of HBM per device.

```python
import math
import jax
import jax.numpy as jnp
from jax import lax

LEV = 137
CHAN = 128
FOOT = 8
COL_DEV = 512
OBS_DEV = 512
HALO = 256
SLOTS = 4
TILES = 8
COLS = 4096
OBS = 16384
N_TM = 4
N_SPACE = 8


def draw_obs_start(key, part):
    total_rows = OBS_DEV * N_TM * N_SPACE
    row_index = jnp.arange(total_rows, dtype=jnp.int32)
    tile_index = row_index // OBS_DEV % N_SPACE
    offset = jax.random.randint(key, (total_rows,), 0, COL_DEV + 2 * HALO - FOOT + 1, dtype=jnp.int32)
    return jnp.mod(tile_index * COL_DEV - HALO + offset, COLS).astype(jnp.int32)


def with_ends(drawn, key, low, top_value):
    longest = drawn.shape.index(max(drawn.shape))
    spots = []
    for shift in (0, 1):
        where = [jax.random.randint(jax.random.fold_in(key, axis), (), 0, length) for axis, length in enumerate(drawn.shape)]
        where[longest] = (where[longest] + shift) % drawn.shape[longest]
        spots.append(tuple(where))
    return drawn.at[spots[0]].set(low).at[spots[1]].set(top_value)


def block_scale(key, extent, split, smallest, largest):
    factor_of = 1.0
    for position, parts in split:
        steps = jax.random.uniform(jax.random.fold_in(jax.random.fold_in(key, 6), position), (parts,), jnp.float32, smallest / len(split), largest / len(split))
        factor_of = factor_of * jnp.repeat(jnp.exp(steps), extent[position] // parts).reshape((-1,) + (1,) * (len(extent) - 1 - position))
    return factor_of


def centred(rng, dims, scale, most, split=(), held_as=jnp.bfloat16):
    array = scale * jax.random.normal(rng, dims, jnp.float32)
    if split:
        array = array * block_scale(rng, dims, split, -0.22, 0.18)
    return jnp.clip(array, -most, most).astype(held_as)


def setup_inputs(seed: int = 0) -> dict:
    streams_of = jax.random.split(jax.random.key(seed), 10)
    state = centred(streams_of[0], (SLOTS, COLS, LEV), 1.0, 6.0, ((0, 4), (1, 8)))
    obs_start = draw_obs_start(jax.random.fold_in(streams_of[9], 71), 0)
    foot_weight = jnp.clip(jnp.exp(math.log(0.29882812) - 2.7092764 * jax.random.uniform(streams_of[2], (OBS, FOOT), jnp.float32) ** block_scale(streams_of[2], (OBS, FOOT), ((0, 32),), -0.2, 0.2)), 0.019897461, 0.29882812).astype(jnp.bfloat16)
    obs_slot = with_ends(jax.random.randint(streams_of[3], (OBS,), 0, SLOTS - 1), jax.random.fold_in(streams_of[3], 1), 0, (SLOTS - 1) - 1).astype(jnp.int32)
    obs_frac = jnp.clip(1.0 * jax.random.uniform(streams_of[4], (OBS,), jnp.float32) ** block_scale(streams_of[4], (OBS,), ((0, 32),), -0.2, 0.2), 0.0, 1.0)
    live_count = with_ends(jax.random.randint(streams_of[5], (SLOTS, TILES), OBS_DEV // 8, OBS_DEV + 1), jax.random.fold_in(streams_of[5], 1), OBS_DEV // 8, OBS_DEV).astype(jnp.int32)
    obs_values = centred(streams_of[6], (OBS, CHAN), 1.0, 6.0, ((0, 32),), jnp.float32)
    jacobian = centred(streams_of[7], (LEV, CHAN), LEV ** -0.5, 0.5)
    inv_var = jnp.clip(jnp.exp(jax.random.uniform(streams_of[8], (CHAN,), jnp.float32, math.log(0.25), math.log(4.0))), 0.25, 4.0)
    return {"state": state, "obs_start": obs_start, "foot_weight": foot_weight, "obs_slot": obs_slot, "obs_frac": obs_frac, "live_count": live_count, "obs_values": obs_values, "jacobian": jacobian, "inv_var": inv_var}


def reference(state, obs_start, foot_weight, obs_slot, obs_frac, live_count, obs_values, jacobian, inv_var):
    cols = state.shape[1]
    groups = live_count.shape[0] * live_count.shape[1]
    per_group = obs_start.shape[0] // groups
    offsets = jnp.arange(FOOT, dtype=jnp.int32)

    def visit(adjoint, inputs):
        start, weight, slot, frac, count, values = inputs
        columns = jnp.mod(start[:, None] + offsets[None, :], cols).astype(jnp.int32)
        lower_slot = slot[:, None].astype(jnp.int32)
        upper_slot = (slot[:, None] + 1).astype(jnp.int32)
        lower = state[lower_slot, columns].astype(jnp.float32)
        upper = state[upper_slot, columns].astype(jnp.float32)
        weight_f = weight.astype(jnp.float32)
        p_lower = jnp.einsum("rk,rkl->rl", weight_f, lower, precision=lax.Precision.HIGHEST)
        p_upper = jnp.einsum("rk,rkl->rl", weight_f, upper, precision=lax.Precision.HIGHEST)
        interp = (1.0 - frac)[:, None] * p_lower + frac[:, None] * p_upper
        projected = jnp.dot(interp.astype(jnp.bfloat16), jacobian, preferred_element_type=jnp.float32)
        live = jnp.arange(per_group, dtype=jnp.int32) < count
        departures = jnp.where(live[:, None], values - projected, jnp.float32(0.0))
        scaled = (departures * inv_var[None, :]).astype(jnp.bfloat16)
        back = jnp.dot(scaled, jnp.transpose(jacobian), preferred_element_type=jnp.float32).astype(jnp.bfloat16)
        back = lax.optimization_barrier(back).astype(jnp.float32)
        v_lower = ((1.0 - frac)[:, None] * back).astype(jnp.bfloat16)
        v_upper = (frac[:, None] * back).astype(jnp.bfloat16)
        v_lower = lax.optimization_barrier(v_lower).astype(jnp.float32)
        v_upper = lax.optimization_barrier(v_upper).astype(jnp.float32)
        adjoint = adjoint.at[lower_slot, columns].add(weight_f[:, :, None] * v_lower[:, None, :])
        adjoint = adjoint.at[upper_slot, columns].add(weight_f[:, :, None] * v_upper[:, None, :])
        return adjoint, departures

    inputs = (
        obs_start.reshape(groups, per_group),
        foot_weight.reshape(groups, per_group, FOOT),
        obs_slot.reshape(groups, per_group),
        obs_frac.reshape(groups, per_group),
        live_count.reshape(groups).astype(jnp.int32),
        obs_values.reshape(groups, per_group, obs_values.shape[1]),
    )
    adjoint, departures = lax.scan(visit, jnp.zeros(state.shape, jnp.float32), inputs)
    return departures.reshape(obs_values.shape), adjoint
```

```python
import functools

import jax
import jax.numpy as jnp
from jax import lax
from jax.experimental import pallas as pl
from jax.experimental.pallas import tpu as pltpu
from jax.sharding import PartitionSpec as P

MESH = pl.DeviceIdType.MESH
F32 = jnp.float32
BF16 = jnp.bfloat16
GROUP = 128
CORES = 2


def nt_dot(a, b):
    return lax.dot_general(a, b, (((1,), (1,)), ((), ())), preferred_element_type=F32)


def nn_dot(a, b):
    return jnp.dot(a, b, preferred_element_type=F32)


def message_names(n_tm, chunks):
    ny = n_tm // CORES
    names = [("meta_i", r) for r in range(1, n_tm)]
    names += [("meta_f", r) for r in range(1, n_tm)]
    names += [("halo", side) for side in range(2)]
    names += [("pair", dy, k) for dy in range(ny) for k in range(chunks)]
    names += [("sum", dy, k) for dy in range(1, ny) for k in range(chunks)]
    names += [("scaled", r, k) for r in range(1, n_tm) for k in range(chunks)]
    names += [("rim", side) for side in range(2)]
    return {name: index for index, name in enumerate(names)}


def kernel(
    n_tm,
    n_space,
    chunks,
    state_ref,
    start_ref,
    weight_ref,
    slot_ref,
    frac_ref,
    live_ref,
    values_ref,
    jac_ref,
    inv_ref,
    dep_ref,
    adj_ref,
    wide,
    meta_i,
    meta_f,
    foot_t,
    partial,
    values_t,
    inv_t,
    pair_out,
    pair_in,
    sum_out,
    sum_in,
    scaled,
    total,
    rim_out,
    rim_in,
    dep_t,
    send_sems,
    recv_sems,
):
    ny = n_tm // CORES
    turn = lax.axis_index("tm")
    tile = lax.axis_index("space")
    row = turn // CORES
    core = lax.rem(turn, CORES)
    left = lax.rem(tile + n_space - 1, n_space)
    right = lax.rem(tile + 1, n_space)
    levels, cols_dev = state_ref.shape
    halo_w = cols_dev // 2
    width = cols_dev + 2 * halo_w
    foot, obs = weight_ref.shape
    chunk_w = obs // chunks
    names = message_names(n_tm, chunks)

    def peer(r):
        dy, dc = r // CORES, r % CORES
        return (lax.rem(row + dy, ny) * CORES + lax.rem(core + dc, CORES), tile)

    def inverse(r):
        return ((ny - r // CORES) % ny) * CORES + r % CORES

    barrier = pltpu.get_barrier_semaphore()
    targets = [(turn, left), (turn, right)] + [peer(r) for r in range(1, n_tm)]
    for target in targets:
        pl.semaphore_signal(barrier, inc=1, device_id=target, device_id_type=MESH)

    started = []

    def send(name, name_there, src, dst, device):
        copy = pltpu.make_async_remote_copy(
            src_ref=src,
            dst_ref=dst,
            send_sem=send_sems.at[names[name]],
            recv_sem=recv_sems.at[names[name_there]],
            device_id=device,
            device_id_type=MESH,
        )
        copy.start()
        started.append(copy)

    def arrived(name, dst, device):
        pltpu.make_async_remote_copy(
            src_ref=dst,
            dst_ref=dst,
            send_sem=send_sems.at[names[name]],
            recv_sem=recv_sems.at[names[name]],
            device_id=device,
            device_id_type=MESH,
        ).wait_recv()

    jac = jac_ref[...]
    chan = jac.shape[1]
    eye = (
        lax.broadcasted_iota(jnp.int32, (chan, chan), 0)
        == lax.broadcasted_iota(jnp.int32, (chan, chan), 1)
    ).astype(F32).astype(BF16)
    jac_t = nt_dot(eye, jac).astype(BF16)
    own = nn_dot(jac_t, state_ref[...]).astype(BF16)
    wide[1] = own[:, :halo_w]
    wide[2] = own[:, halo_w:]

    total_cols = cols_dev * n_space
    local = start_ref[...] - tile * cols_dev + halo_w
    local = jnp.where(local < 0, local + total_cols, local)
    local = jnp.where(local >= total_cols, local - total_cols, local)
    meta_i[0, 0:1] = local
    meta_i[0, 1:2] = slot_ref[...]
    frac = frac_ref[...]
    weight = weight_ref[...].astype(F32)
    meta_f[0] = jnp.concatenate([weight * (1.0 - frac), weight * frac], axis=0).astype(BF16)

    pl.semaphore_wait(barrier, len(targets))
    send(("halo", 0), ("halo", 1), wide.at[1], wide.at[3], (turn, left))
    send(("halo", 1), ("halo", 0), wide.at[2], wide.at[0], (turn, right))
    for r in range(1, n_tm):
        back = inverse(r)
        send(("meta_i", r), ("meta_i", back), meta_i.at[0], meta_i.at[back], peer(r))
        send(("meta_f", r), ("meta_f", back), meta_f.at[0], meta_f.at[back], peer(r))

    def build(r):
        start = meta_i[r, 0:1]
        slot = meta_i[r, 1:2]
        pairs = meta_f[r].astype(F32)
        weights = jnp.where(slot == turn, pairs[:foot], 0.0)
        weights = weights + jnp.where(slot + 1 == turn, pairs[foot:], 0.0)
        place = lax.broadcasted_iota(jnp.int32, (GROUP, obs), 0)
        offset = jnp.bitwise_and(place - start, GROUP - 1)
        group = jnp.right_shift(start + offset, 7)
        value = jnp.zeros((GROUP, obs), F32)
        for k in range(foot):
            value = jnp.where(offset == k, weights[k : k + 1], value)
        for j in range(width // GROUP):
            block = jnp.where(group == j, value, 0.0).astype(BF16)
            foot_t[r, j * GROUP : (j + 1) * GROUP, :] = block

    def project(r, b):
        return nn_dot(wide[b], foot_t[r, b * halo_w : (b + 1) * halo_w, :])

    build(0)
    partial[0] = project(0, 1) + project(0, 2)
    values_t[...] = values_ref[...].T
    inv_t[...] = jnp.broadcast_to(inv_ref[...], (GROUP, chan)).T
    order = [r for r in range(1, n_tm)]
    for r in order:
        arrived(("meta_i", r), meta_i.at[r], peer(r))
        arrived(("meta_f", r), meta_f.at[r], peer(r))
        build(r)
        partial[r] = project(r, 1) + project(r, 2)

    arrived(("halo", 0), wide.at[0], (turn, left))
    arrived(("halo", 1), wide.at[3], (turn, right))

    def finish(r, k):
        lanes = slice(k * chunk_w, (k + 1) * chunk_w)
        edge = nn_dot(wide[0], foot_t[r, 0:halo_w, lanes])
        edge = edge + nn_dot(wide[3], foot_t[r, width - halo_w :, lanes])
        return partial[r, :, lanes] + edge

    for dy in range(1, ny):
        for k in range(chunks):
            pair_out[dy, k] = finish(dy * CORES + 1, k).astype(BF16)
            send(("pair", dy, k), ("pair", dy, k), pair_out.at[dy, k], pair_in.at[dy, k], peer(1))
    for dy in range(1, ny):
        back = ny - dy
        for k in range(chunks):
            mine = finish(dy * CORES, k)
            arrived(("pair", dy, k), pair_in.at[dy, k], peer(1))
            sum_out[dy, k] = (mine + pair_in[dy, k].astype(F32)).astype(BF16)
            send(("sum", dy, k), ("sum", back, k), sum_out.at[dy, k], sum_in.at[back, k], peer(dy * CORES))
    for k in range(chunks):
        pair_out[0, k] = finish(1, k).astype(BF16)
        send(("pair", 0, k), ("pair", 0, k), pair_out.at[0, k], pair_in.at[0, k], peer(1))
    for k in range(chunks):
        lanes = slice(k * chunk_w, (k + 1) * chunk_w)
        partial[0, :, lanes] = finish(0, k)
    for k in range(chunks):
        lanes = slice(k * chunk_w, (k + 1) * chunk_w)
        arrived(("pair", 0, k), pair_in.at[0, k], peer(1))
        projected = partial[0, :, lanes] + pair_in[0, k].astype(F32)
        for dy in range(1, ny):
            arrived(("sum", dy, k), sum_in.at[dy, k], peer(dy * CORES))
            projected = projected + sum_in[dy, k].astype(F32)
        place = lax.broadcasted_iota(jnp.int32, (chan, chunk_w), 1) + k * chunk_w
        departure = jnp.where(place < live_ref[0, 0], values_t[:, lanes] - projected, 0.0)
        dep_t[:, lanes] = departure
        scale = jnp.concatenate([inv_t[...]] * (chunk_w // GROUP), axis=1)
        scaled[0, k] = (departure * scale).astype(BF16)
        for dy in range(1, ny):
            r = dy * CORES
            back = inverse(r)
            send(("scaled", r, k), ("scaled", back, k), scaled.at[0, k], scaled.at[back, k], peer(r))
        send(("scaled", 1, k), ("scaled", 1, k), scaled.at[0, k], scaled.at[1, k], peer(1))

    def spread(r, k, b):
        lanes = slice(k * chunk_w, (k + 1) * chunk_w)
        return nt_dot(scaled[r, k], foot_t[r, b * halo_w : (b + 1) * halo_w, lanes])

    dep_ref[...] = dep_t[...].T
    for b in range(4):
        here = spread(0, 0, b)
        for k in range(1, chunks):
            here = here + spread(0, k, b)
        total[b] = here
    for k in range(chunks):
        arrived(("scaled", 1, k), scaled.at[1, k], peer(1))
    for b in range(4):
        here = total[b]
        for k in range(chunks):
            here = here + spread(1, k, b)
        total[b] = here
    for k in range(chunks):
        for dy in range(1, ny):
            r = dy * CORES
            arrived(("scaled", r, k), scaled.at[r, k], peer(r))
            send(("scaled", r + 1, k), ("scaled", r + 1, k), scaled.at[r, k], scaled.at[r + 1, k], peer(1))
        for dy in range(1, ny):
            for b in range(4):
                total[b] = total[b] + spread(dy * CORES, k, b)
    for dy in range(1, ny):
        for k in range(chunks):
            arrived(("scaled", dy * CORES + 1, k), scaled.at[dy * CORES + 1, k], peer(1))

    def last(b):
        here = total[b]
        for dy in range(1, ny):
            for k in range(chunks):
                here = here + spread(dy * CORES + 1, k, b)
        return here

    rim_out[0] = last(0).astype(BF16)
    send(("rim", 0), ("rim", 1), rim_out.at[0], rim_in.at[1], (turn, left))
    rim_out[1] = last(3).astype(BF16)
    send(("rim", 1), ("rim", 0), rim_out.at[1], rim_in.at[0], (turn, right))
    core_sums = [last(1), last(2)]
    for side in range(2):
        arrived(("rim", side), rim_in.at[side], (turn, (left, right)[side]))
        columns = (core_sums[side] + rim_in[side].astype(F32)).astype(BF16)
        adj_ref[:, side * halo_w : (side + 1) * halo_w] = nn_dot(jac, columns)
    for copy in started:
        copy.wait_send()


def body(
    state, obs_start, foot_weight, obs_slot, obs_frac, live_count, obs_values, jacobian, inv_var
):
    n_tm = lax.axis_size("tm")
    n_space = lax.axis_size("space")
    ny = n_tm // CORES
    chunks = 2
    _, cols_dev, levels = state.shape
    obs, chan = obs_values.shape
    foot = foot_weight.shape[1]
    halo_w = cols_dev // 2
    width = cols_dev + 2 * halo_w
    chunk_w = obs // chunks
    vmem = pl.BlockSpec(memory_space=pltpu.VMEM)
    smem = pl.BlockSpec(memory_space=pltpu.SMEM)
    count = len(message_names(n_tm, chunks))
    departures, adjoint_t = pl.pallas_call(
        functools.partial(kernel, n_tm, n_space, chunks),
        name="departures_and_adjoint",
        out_shape=(
            jax.ShapeDtypeStruct((obs, chan), F32),
            jax.ShapeDtypeStruct((levels, cols_dev), F32),
        ),
        in_specs=[vmem, vmem, vmem, vmem, vmem, smem, vmem, vmem, vmem],
        out_specs=(vmem, vmem),
        scratch_shapes=[
            pltpu.VMEM((4, chan, halo_w), BF16),
            pltpu.VMEM((n_tm, 2, obs), jnp.int32),
            pltpu.VMEM((n_tm, 2 * foot, obs), BF16),
            pltpu.VMEM((n_tm, width, obs), BF16),
            pltpu.VMEM((n_tm, chan, obs), F32),
            pltpu.VMEM((chan, obs), F32),
            pltpu.VMEM((chan, GROUP), F32),
            pltpu.VMEM((ny, chunks, chan, chunk_w), BF16),
            pltpu.VMEM((ny, chunks, chan, chunk_w), BF16),
            pltpu.VMEM((ny, chunks, chan, chunk_w), BF16),
            pltpu.VMEM((ny, chunks, chan, chunk_w), BF16),
            pltpu.VMEM((n_tm, chunks, chan, chunk_w), BF16),
            pltpu.VMEM((4, chan, halo_w), F32),
            pltpu.VMEM((2, chan, halo_w), BF16),
            pltpu.VMEM((2, chan, halo_w), BF16),
            pltpu.VMEM((chan, obs), F32),
            pltpu.SemaphoreType.DMA((count,)),
            pltpu.SemaphoreType.DMA((count,)),
        ],
        compiler_params=pltpu.CompilerParams(
            collective_id=0, has_side_effects=True, vmem_limit_bytes=48 * 1024 * 1024
        ),
    )(
        state[0].T,
        obs_start[None],
        foot_weight.T,
        obs_slot[None],
        obs_frac[None],
        live_count,
        obs_values,
        jacobian,
        inv_var[None],
    )
    return (departures, adjoint_t.T[None])


def solution(mesh):
    return jax.shard_map(
        body,
        mesh=mesh,
        in_specs=(
            P("tm", "space", None),
            P(("tm", "space")),
            P(("tm", "space"), None),
            P(("tm", "space")),
            P(("tm", "space")),
            P("tm", "space"),
            P(("tm", "space"), None),
            P(),
            P(),
        ),
        out_specs=(P(("tm", "space"), None), P("tm", "space", None)),
        check_vma=False,
    )
```

```python
import functools

import jax
import jax.numpy as jnp
from jax import lax
from jax.experimental import pallas as pl
from jax.experimental.pallas import tpu as pltpu
from jax.sharding import PartitionSpec as P

MESH = pl.DeviceIdType.MESH
F32 = jnp.float32
BF16 = jnp.bfloat16
GROUP = 128
CORES = 2


def nt_dot(a, b):
    return lax.dot_general(a, b, (((1,), (1,)), ((), ())), preferred_element_type=F32)


def nn_dot(a, b):
    return jnp.dot(a, b, preferred_element_type=F32)


def message_names(n_tm, chunks):
    ny = n_tm // CORES
    names = [("meta_i", r) for r in range(1, n_tm)]
    names += [("meta_f", r) for r in range(1, n_tm)]
    names += [("halo", side) for side in range(2)]
    names += [("pair", dy, k) for dy in range(ny) for k in range(chunks)]
    names += [("sum", dy, k) for dy in range(1, ny) for k in range(chunks)]
    names += [("scaled", r, k) for r in range(1, n_tm) for k in range(chunks)]
    names += [("rim", side) for side in range(2)]
    return {name: index for index, name in enumerate(names)}


def kernel(
    n_tm,
    n_space,
    chunks,
    state_hbm,
    start_hbm,
    weight_hbm,
    slot_hbm,
    frac_hbm,
    live_ref,
    values_hbm,
    jac_hbm,
    inv_hbm,
    dep_ref,
    sum_ref,
    state_ref,
    start_ref,
    weight_ref,
    slot_ref,
    frac_ref,
    values_ref,
    jac_ref,
    inv_ref,
    wide,
    meta_i,
    meta_f,
    foot_t,
    partial,
    values_t,
    inv_t,
    pair_out,
    pair_in,
    sum_out,
    sum_in,
    scaled,
    total,
    rim_out,
    rim_in,
    dep_t,
    load_sems,
    send_sems,
    recv_sems,
):
    ny = n_tm // CORES
    turn = lax.axis_index("tm")
    tile = lax.axis_index("space")
    row = turn // CORES
    core = lax.rem(turn, CORES)
    left = lax.rem(tile + n_space - 1, n_space)
    right = lax.rem(tile + 1, n_space)
    levels, cols_dev = state_ref.shape
    halo_w = cols_dev // 2
    width = cols_dev + 2 * halo_w
    foot, obs = weight_ref.shape
    chunk_w = obs // chunks
    names = message_names(n_tm, chunks)

    def peer(r):
        dy, dc = r // CORES, r % CORES
        return (lax.rem(row + dy, ny) * CORES + lax.rem(core + dc, CORES), tile)

    def inverse(r):
        return ((ny - r // CORES) % ny) * CORES + r % CORES

    barrier = pltpu.get_barrier_semaphore()
    targets = [(turn, left), (turn, right)] + [peer(r) for r in range(1, n_tm)]
    for target in targets:
        pl.semaphore_signal(barrier, inc=1, device_id=target, device_id_type=MESH)

    pairs_in = [
        (state_hbm, state_ref),
        (jac_hbm, jac_ref),
        (start_hbm, start_ref),
        (slot_hbm, slot_ref),
        (frac_hbm, frac_ref),
        (weight_hbm, weight_ref),
        (inv_hbm, inv_ref),
        (values_hbm, values_ref),
    ]
    loads = [
        pltpu.make_async_copy(src, dst, load_sems.at[i]) for i, (src, dst) in enumerate(pairs_in)
    ]
    for load in loads:
        load.start()

    started = []

    def send(name, name_there, src, dst, device):
        send_at(names[name], names[name_there], src, dst, device)

    def send_at(index, index_there, src, dst, device):
        copy = pltpu.make_async_remote_copy(
            src_ref=src,
            dst_ref=dst,
            send_sem=send_sems.at[index],
            recv_sem=recv_sems.at[index_there],
            device_id=device,
            device_id_type=MESH,
        )
        copy.start()
        started.append(copy)

    def arrived(name, dst, device):
        pltpu.make_async_remote_copy(
            src_ref=dst,
            dst_ref=dst,
            send_sem=send_sems.at[names[name]],
            recv_sem=recv_sems.at[names[name]],
            device_id=device,
            device_id_type=MESH,
        ).wait_recv()

    def send_sides(name, sources, targets_there, source_index, target_index):
        odd = lax.rem(tile, 2)
        for side in (odd, 1 - odd):
            device = (turn, lax.rem(tile + n_space - 1 + 2 * side, n_space))
            base = names[(name, 0)]
            send_at(
                base + side,
                base + 1 - side,
                sources.at[source_index(side)],
                targets_there.at[target_index(side)],
                device,
            )

    for load in loads[2:6]:
        load.wait()
    total_cols = cols_dev * n_space
    local = start_ref[...] - tile * cols_dev + halo_w
    local = jnp.where(local < 0, local + total_cols, local)
    local = jnp.where(local >= total_cols, local - total_cols, local)
    meta_i[0, 0:1] = local
    meta_i[0, 1:2] = slot_ref[...]
    frac = frac_ref[...]
    weight = weight_ref[...].astype(F32)
    meta_f[0] = jnp.concatenate([weight * (1.0 - frac), weight * frac], axis=0).astype(BF16)
    for load in loads[:2]:
        load.wait()

    jac = jac_ref[...]
    chan = jac.shape[1]
    eye = (
        lax.broadcasted_iota(jnp.int32, (chan, chan), 0)
        == lax.broadcasted_iota(jnp.int32, (chan, chan), 1)
    ).astype(F32).astype(BF16)
    jac_t = nt_dot(eye, jac).astype(BF16)
    own = nn_dot(jac_t, state_ref[...]).astype(BF16)
    wide[1] = own[:, :halo_w]
    wide[2] = own[:, halo_w:]

    pl.semaphore_wait(barrier, len(targets))
    send_sides("halo", wide, wide, lambda side: 1 + side, lambda side: 3 - 3 * side)
    for r in range(1, n_tm):
        back = inverse(r)
        send(("meta_i", r), ("meta_i", back), meta_i.at[0], meta_i.at[back], peer(r))
        send(("meta_f", r), ("meta_f", back), meta_f.at[0], meta_f.at[back], peer(r))

    def build(r):
        start = meta_i[r, 0:1]
        slot = meta_i[r, 1:2]
        pairs = meta_f[r].astype(F32)
        weights = jnp.where(slot == turn, pairs[:foot], 0.0)
        weights = weights + jnp.where(slot + 1 == turn, pairs[foot:], 0.0)
        place = lax.broadcasted_iota(jnp.int32, (GROUP, obs), 0)
        offset = jnp.bitwise_and(place - start, GROUP - 1)
        group = jnp.right_shift(start + offset, 7)
        value = jnp.zeros((GROUP, obs), F32)
        for k in range(foot):
            value = jnp.where(offset == k, weights[k : k + 1], value)
        for j in range(width // GROUP):
            block = jnp.where(group == j, value, 0.0).astype(BF16)
            foot_t[r, j * GROUP : (j + 1) * GROUP, :] = block

    def project(r, b):
        return nn_dot(wide[b], foot_t[r, b * halo_w : (b + 1) * halo_w, :])

    build(0)
    partial[0] = project(0, 1) + project(0, 2)
    for load in loads[6:]:
        load.wait()
    values_t[...] = values_ref[...].T
    inv_t[...] = jnp.broadcast_to(inv_ref[...], (GROUP, chan)).T
    order = [r for r in range(1, n_tm)]
    for r in order:
        arrived(("meta_i", r), meta_i.at[r], peer(r))
        arrived(("meta_f", r), meta_f.at[r], peer(r))
        build(r)
        partial[r] = project(r, 1) + project(r, 2)

    arrived(("halo", 0), wide.at[0], (turn, left))
    arrived(("halo", 1), wide.at[3], (turn, right))

    def finish(r, k):
        lanes = slice(k * chunk_w, (k + 1) * chunk_w)
        edge = nn_dot(wide[0], foot_t[r, 0:halo_w, lanes])
        edge = edge + nn_dot(wide[3], foot_t[r, width - halo_w :, lanes])
        return partial[r, :, lanes] + edge

    for dy in range(1, ny):
        for k in range(chunks):
            pair_out[dy, k] = finish(dy * CORES + 1, k).astype(BF16)
            send(("pair", dy, k), ("pair", dy, k), pair_out.at[dy, k], pair_in.at[dy, k], peer(1))
    for dy in range(1, ny):
        back = ny - dy
        for k in range(chunks):
            mine = finish(dy * CORES, k)
            arrived(("pair", dy, k), pair_in.at[dy, k], peer(1))
            sum_out[dy, k] = (mine + pair_in[dy, k].astype(F32)).astype(BF16)
            send(("sum", dy, k), ("sum", back, k), sum_out.at[dy, k], sum_in.at[back, k], peer(dy * CORES))
    for k in range(chunks):
        pair_out[0, k] = finish(1, k).astype(BF16)
        send(("pair", 0, k), ("pair", 0, k), pair_out.at[0, k], pair_in.at[0, k], peer(1))
    for k in range(chunks):
        lanes = slice(k * chunk_w, (k + 1) * chunk_w)
        partial[0, :, lanes] = finish(0, k)
    for k in range(chunks):
        lanes = slice(k * chunk_w, (k + 1) * chunk_w)
        arrived(("pair", 0, k), pair_in.at[0, k], peer(1))
        projected = partial[0, :, lanes] + pair_in[0, k].astype(F32)
        for dy in range(1, ny):
            arrived(("sum", dy, k), sum_in.at[dy, k], peer(dy * CORES))
            projected = projected + sum_in[dy, k].astype(F32)
        place = lax.broadcasted_iota(jnp.int32, (chan, chunk_w), 1) + k * chunk_w
        departure = jnp.where(place < live_ref[0, 0], values_t[:, lanes] - projected, 0.0)
        dep_t[:, lanes] = departure
        scale = jnp.concatenate([inv_t[...]] * (chunk_w // GROUP), axis=1)
        scaled[0, k] = (departure * scale).astype(BF16)
        for dy in range(1, ny):
            r = dy * CORES
            back = inverse(r)
            send(("scaled", r, k), ("scaled", back, k), scaled.at[0, k], scaled.at[back, k], peer(r))
        send(("scaled", 1, k), ("scaled", 1, k), scaled.at[0, k], scaled.at[1, k], peer(1))

    def spread(r, k, b):
        lanes = slice(k * chunk_w, (k + 1) * chunk_w)
        return nt_dot(scaled[r, k], foot_t[r, b * halo_w : (b + 1) * halo_w, lanes])

    dep_ref[...] = dep_t[...].T
    for b in range(4):
        here = spread(0, 0, b)
        for k in range(1, chunks):
            here = here + spread(0, k, b)
        total[b] = here
    for k in range(chunks):
        arrived(("scaled", 1, k), scaled.at[1, k], peer(1))
    for b in range(4):
        here = total[b]
        for k in range(chunks):
            here = here + spread(1, k, b)
        total[b] = here
    for k in range(chunks):
        for dy in range(1, ny):
            r = dy * CORES
            arrived(("scaled", r, k), scaled.at[r, k], peer(r))
            send(("scaled", r + 1, k), ("scaled", r + 1, k), scaled.at[r, k], scaled.at[r + 1, k], peer(1))
        for dy in range(1, ny):
            for b in range(4):
                total[b] = total[b] + spread(dy * CORES, k, b)
    for dy in range(1, ny):
        for k in range(chunks):
            arrived(("scaled", dy * CORES + 1, k), scaled.at[dy * CORES + 1, k], peer(1))

    def last(b):
        here = total[b]
        for dy in range(1, ny):
            for k in range(chunks):
                here = here + spread(dy * CORES + 1, k, b)
        return here

    rim_out[0] = last(0).astype(BF16)
    rim_out[1] = last(3).astype(BF16)
    send_sides("rim", rim_out, rim_in, lambda side: side, lambda side: 1 - side)
    core_sums = [last(1), last(2)]
    for side in range(2):
        arrived(("rim", side), rim_in.at[side], (turn, (left, right)[side]))
        sum_ref[side] = (core_sums[side] + rim_in[side].astype(F32)).astype(BF16)
    for copy in started:
        copy.wait_send()


def finish_kernel(dep_ref, sum_ref, jac_ref, dep_hbm, adj_hbm, adj_ref, sems):
    dep_copy = pltpu.make_async_copy(dep_ref, dep_hbm, sems.at[0])
    dep_copy.start()
    jac = jac_ref[...]
    levels = jac.shape[0]
    halo_w = sum_ref.shape[2]
    for side in range(2):
        lanes = slice(side * halo_w, (side + 1) * halo_w)
        adj_ref[:, :, lanes] = nn_dot(jac, sum_ref[side]).reshape(levels, 1, halo_w)
    adj_copy = pltpu.make_async_copy(adj_ref, adj_hbm, sems.at[1])
    adj_copy.start()
    dep_copy.wait()
    adj_copy.wait()


def body(
    state, obs_start, foot_weight, obs_slot, obs_frac, live_count, obs_values, jacobian, inv_var
):
    n_tm = lax.axis_size("tm")
    n_space = lax.axis_size("space")
    ny = n_tm // CORES
    chunks = 4
    _, cols_dev, levels = state.shape
    obs, chan = obs_values.shape
    foot = foot_weight.shape[1]
    halo_w = cols_dev // 2
    width = cols_dev + 2 * halo_w
    chunk_w = obs // chunks
    vmem = pl.BlockSpec(memory_space=pltpu.VMEM)
    live_space = pl.BlockSpec(memory_space=pltpu.SMEM)
    hbm = pl.BlockSpec(memory_space=pltpu.HBM)
    count = len(message_names(n_tm, chunks))
    departures, sums = pl.pallas_call(
        functools.partial(kernel, n_tm, n_space, chunks),
        name="departures_and_adjoint",
        out_shape=(
            pltpu.VMEM((obs, chan), F32),
            pltpu.VMEM((2, chan, halo_w), BF16),
        ),
        in_specs=[hbm] * 5 + [live_space] + [hbm] * 3,
        out_specs=(vmem, vmem),
        scratch_shapes=[
            pltpu.VMEM((levels, cols_dev), BF16),
            pltpu.VMEM((1, obs), jnp.int32),
            pltpu.VMEM((foot, obs), BF16),
            pltpu.VMEM((1, obs), jnp.int32),
            pltpu.VMEM((1, obs), F32),
            pltpu.VMEM((obs, chan), F32),
            pltpu.VMEM((levels, chan), BF16),
            pltpu.VMEM((1, chan), F32),
            pltpu.VMEM((4, chan, halo_w), BF16),
            pltpu.VMEM((n_tm, 2, obs), jnp.int32),
            pltpu.VMEM((n_tm, 2 * foot, obs), BF16),
            pltpu.VMEM((n_tm, width, obs), BF16),
            pltpu.VMEM((n_tm, chan, obs), F32),
            pltpu.VMEM((chan, obs), F32),
            pltpu.VMEM((chan, GROUP), F32),
            pltpu.VMEM((ny, chunks, chan, chunk_w), BF16),
            pltpu.VMEM((ny, chunks, chan, chunk_w), BF16),
            pltpu.VMEM((ny, chunks, chan, chunk_w), BF16),
            pltpu.VMEM((ny, chunks, chan, chunk_w), BF16),
            pltpu.VMEM((n_tm, chunks, chan, chunk_w), BF16),
            pltpu.VMEM((4, chan, halo_w), F32),
            pltpu.VMEM((2, chan, halo_w), BF16),
            pltpu.VMEM((2, chan, halo_w), BF16),
            pltpu.VMEM((chan, obs), F32),
            pltpu.SemaphoreType.DMA((8,)),
            pltpu.SemaphoreType.DMA((count,)),
            pltpu.SemaphoreType.DMA((count,)),
        ],
        compiler_params=pltpu.CompilerParams(
            collective_id=0, has_side_effects=True, vmem_limit_bytes=58 * 1024 * 1024
        ),
    )(
        state[0].T,
        obs_start[None],
        foot_weight.T,
        obs_slot[None],
        obs_frac[None],
        live_count,
        obs_values,
        jacobian,
        inv_var[None],
    )
    departures, adjoint_t = pl.pallas_call(
        finish_kernel,
        name="write_outputs",
        out_shape=(
            jax.ShapeDtypeStruct((obs, chan), F32),
            jax.ShapeDtypeStruct((levels, 1, cols_dev), F32),
        ),
        in_specs=[vmem, vmem, vmem],
        out_specs=(hbm, hbm),
        scratch_shapes=[
            pltpu.VMEM((levels, 1, cols_dev), F32),
            pltpu.SemaphoreType.DMA((2,)),
        ],
        compiler_params=pltpu.CompilerParams(vmem_limit_bytes=4 * 1024 * 1024),
    )(departures, sums, jacobian)
    return (departures, adjoint_t.transpose(1, 2, 0))


def solution(mesh):
    return jax.shard_map(
        body,
        mesh=mesh,
        in_specs=(
            P("tm", "space", None),
            P(("tm", "space")),
            P(("tm", "space"), None),
            P(("tm", "space")),
            P(("tm", "space")),
            P("tm", "space"),
            P(("tm", "space"), None),
            P(),
            P(),
        ),
        out_specs=(P(("tm", "space"), None), P("tm", "space", None)),
        check_vma=False,
    )
```

```python
import functools

import jax
import jax.numpy as jnp
from jax import lax
from jax.experimental import pallas as pl
from jax.experimental.pallas import tpu as pltpu
from jax.sharding import PartitionSpec as P

MESH = pl.DeviceIdType.MESH
F32 = jnp.float32
BF16 = jnp.bfloat16
GROUP = 128
CORES = 2


def nt_dot(a, b):
    return lax.dot_general(a, b, (((1,), (1,)), ((), ())), preferred_element_type=F32)


def nn_dot(a, b):
    return jnp.dot(a, b, preferred_element_type=F32)


def message_names(n_tm, chunks):
    ny = n_tm // CORES
    names = [("meta_i", r) for r in range(1, n_tm)]
    names += [("meta_f", r) for r in range(1, n_tm)]
    names += [("halo", k, side) for k in range(chunks) for side in range(2)]
    names += [("pair", dy, k) for dy in range(ny) for k in range(chunks)]
    names += [("sum", dy, k) for dy in range(1, ny) for k in range(chunks)]
    names += [("scaled", r, k) for r in range(1, n_tm) for k in range(chunks)]
    names += [("rim", k, side) for k in range(chunks) for side in range(2)]
    return {name: index for index, name in enumerate(names)}


def kernel(
    n_tm,
    n_space,
    chunks,
    state_hbm,
    start_hbm,
    weight_hbm,
    slot_hbm,
    frac_hbm,
    live_ref,
    values_hbm,
    jac_hbm,
    inv_hbm,
    dep_ref,
    sum_ref,
    state_ref,
    start_ref,
    weight_ref,
    slot_ref,
    frac_ref,
    values_ref,
    jac_ref,
    inv_ref,
    wide,
    meta_i,
    meta_f,
    foot_t,
    partial,
    values_t,
    inv_t,
    pair_out,
    pair_in,
    sum_out,
    sum_in,
    scaled,
    total,
    rim_out,
    rim_in,
    dep_t,
    load_sems,
    send_sems,
    recv_sems,
):
    ny = n_tm // CORES
    turn = lax.axis_index("tm")
    tile = lax.axis_index("space")
    row = turn // CORES
    core = lax.rem(turn, CORES)
    left = lax.rem(tile + n_space - 1, n_space)
    right = lax.rem(tile + 1, n_space)
    levels, cols_dev = state_ref.shape
    halo_w = cols_dev // 2
    width = cols_dev + 2 * halo_w
    foot, obs = weight_ref.shape
    names = message_names(n_tm, chunks)

    def peer(r):
        dy, dc = r // CORES, r % CORES
        return (lax.rem(row + dy, ny) * CORES + lax.rem(core + dc, CORES), tile)

    def inverse(r):
        return ((ny - r // CORES) % ny) * CORES + r % CORES

    barrier = pltpu.get_barrier_semaphore()
    targets = [(turn, left), (turn, right)] + [peer(r) for r in range(1, n_tm)]
    for target in targets:
        pl.semaphore_signal(barrier, inc=1, device_id=target, device_id_type=MESH)

    pairs_in = [
        (state_hbm, state_ref),
        (jac_hbm, jac_ref),
        (start_hbm, start_ref),
        (slot_hbm, slot_ref),
        (frac_hbm, frac_ref),
        (weight_hbm, weight_ref),
        (inv_hbm, inv_ref),
        (values_hbm, values_ref),
    ]
    loads = [
        pltpu.make_async_copy(src, dst, load_sems.at[i]) for i, (src, dst) in enumerate(pairs_in)
    ]
    for load in loads:
        load.start()

    started = []

    def send(name, name_there, src, dst, device):
        send_at(names[name], names[name_there], src, dst, device)

    def send_at(index, index_there, src, dst, device):
        copy = pltpu.make_async_remote_copy(
            src_ref=src,
            dst_ref=dst,
            send_sem=send_sems.at[index],
            recv_sem=recv_sems.at[index_there],
            device_id=device,
            device_id_type=MESH,
        )
        copy.start()
        started.append(copy)

    def arrived(name, dst, device):
        pltpu.make_async_remote_copy(
            src_ref=dst,
            dst_ref=dst,
            send_sem=send_sems.at[names[name]],
            recv_sem=recv_sems.at[names[name]],
            device_id=device,
            device_id_type=MESH,
        ).wait_recv()

    def send_sides(name, k, sources, targets_there, source_index, target_index):
        odd = lax.rem(tile, 2)
        for side in (odd, 1 - odd):
            device = (turn, lax.rem(tile + n_space - 1 + 2 * side, n_space))
            base = names[(name, k, 0)]
            send_at(
                base + side,
                base + 1 - side,
                sources.at[source_index(side), k],
                targets_there.at[target_index(side), k],
                device,
            )

    for load in loads[2:6]:
        load.wait()
    total_cols = cols_dev * n_space
    local = start_ref[...] - tile * cols_dev + halo_w
    local = jnp.where(local < 0, local + total_cols, local)
    local = jnp.where(local >= total_cols, local - total_cols, local)
    meta_i[0, 0:1] = local
    meta_i[0, 1:2] = slot_ref[...]
    frac = frac_ref[...]
    weight = weight_ref[...].astype(F32)
    meta_f[0] = jnp.concatenate([weight * (1.0 - frac), weight * frac], axis=0).astype(BF16)
    for load in loads[:2]:
        load.wait()

    jac = jac_ref[...]
    chan = jac.shape[1]
    eye = (
        lax.broadcasted_iota(jnp.int32, (chan, chan), 0)
        == lax.broadcasted_iota(jnp.int32, (chan, chan), 1)
    ).astype(F32).astype(BF16)
    jac_t = nt_dot(eye, jac).astype(BF16)
    own = nn_dot(jac_t, state_ref[...]).astype(BF16)
    rows = chan // chunks
    for k in range(chunks):
        wide[1, k] = own[k * rows : (k + 1) * rows, :halo_w]
        wide[2, k] = own[k * rows : (k + 1) * rows, halo_w:]

    pl.semaphore_wait(barrier, len(targets))
    for k in range(chunks):
        send_sides("halo", k, wide, wide, lambda side: 1 + side, lambda side: 3 - 3 * side)
    for r in range(1, n_tm):
        back = inverse(r)
        send(("meta_i", r), ("meta_i", back), meta_i.at[0], meta_i.at[back], peer(r))
        send(("meta_f", r), ("meta_f", back), meta_f.at[0], meta_f.at[back], peer(r))

    def build(r):
        start = meta_i[r, 0:1]
        slot = meta_i[r, 1:2]
        pairs = meta_f[r].astype(F32)
        weights = jnp.where(slot == turn, pairs[:foot], 0.0)
        weights = weights + jnp.where(slot + 1 == turn, pairs[foot:], 0.0)
        place = lax.broadcasted_iota(jnp.int32, (GROUP, obs), 0)
        offset = jnp.bitwise_and(place - start, GROUP - 1)
        group = jnp.right_shift(start + offset, 7)
        value = jnp.zeros((GROUP, obs), F32)
        for k in range(foot):
            value = jnp.where(offset == k, weights[k : k + 1], value)
        for j in range(width // GROUP):
            block = jnp.where(group == j, value, 0.0).astype(BF16)
            foot_t[r, j * GROUP : (j + 1) * GROUP, :] = block

    def project(r, b):
        return nn_dot(wide[b].reshape(chan, halo_w), foot_t[r, b * halo_w : (b + 1) * halo_w, :])

    build(0)
    partial[0] = project(0, 1) + project(0, 2)
    for load in loads[6:]:
        load.wait()
    values_t[...] = values_ref[...].T
    inv_t[...] = jnp.broadcast_to(inv_ref[...], (GROUP, chan)).T
    order = [r for r in range(1, n_tm)]
    for r in order:
        arrived(("meta_i", r), meta_i.at[r], peer(r))
        arrived(("meta_f", r), meta_f.at[r], peer(r))
        build(r)
        partial[r] = project(r, 1) + project(r, 2)

    def finish(r, k):
        edge = nn_dot(wide[0, k], foot_t[r, 0:halo_w, :])
        edge = edge + nn_dot(wide[3, k], foot_t[r, width - halo_w :, :])
        partial[r, k * rows : (k + 1) * rows, :] += edge
        return partial[r, k * rows : (k + 1) * rows, :]

    def send_pair(dy, k):
        pair_out[dy, k] = finish(dy * CORES + 1, k).astype(BF16)
        send(("pair", dy, k), ("pair", dy, k), pair_out.at[dy, k], pair_in.at[dy, k], peer(1))

    def send_sum(k):
        for dy in range(1, ny):
            back = ny - dy
            arrived(("pair", dy, k), pair_in.at[dy, k], peer(1))
            mine = partial[dy * CORES, k * rows : (k + 1) * rows, :]
            sum_out[dy, k] = (mine + pair_in[dy, k].astype(F32)).astype(BF16)
            send(("sum", dy, k), ("sum", back, k), sum_out.at[dy, k], sum_in.at[back, k], peer(dy * CORES))

    for k in range(chunks):
        arrived(("halo", k, 0), wide.at[0, k], (turn, left))
        arrived(("halo", k, 1), wide.at[3, k], (turn, right))
        for dy in range(1, ny):
            send_pair(dy, k)
        for dy in range(1, ny):
            finish(dy * CORES, k)
        if k > 0:
            send_sum(k - 1)
    send_sum(chunks - 1)
    for k in range(chunks):
        send_pair(0, k)
    for k in range(chunks):
        finish(0, k)

    for k in range(chunks):
        part = slice(k * rows, (k + 1) * rows)
        arrived(("pair", 0, k), pair_in.at[0, k], peer(1))
        projected = partial[0, part, :] + pair_in[0, k].astype(F32)
        for dy in range(1, ny):
            arrived(("sum", dy, k), sum_in.at[dy, k], peer(dy * CORES))
            projected = projected + sum_in[dy, k].astype(F32)
        place = lax.broadcasted_iota(jnp.int32, (rows, obs), 1)
        departure = jnp.where(place < live_ref[0, 0], values_t[part, :] - projected, 0.0)
        dep_t[part, :] = departure
        scale = jnp.concatenate([inv_t[part, :]] * (obs // GROUP), axis=1)
        scaled[0, k] = (departure * scale).astype(BF16)
        for dy in range(1, ny):
            r = dy * CORES
            back = inverse(r)
            send(("scaled", r, k), ("scaled", back, k), scaled.at[0, k], scaled.at[back, k], peer(r))
        send(("scaled", 1, k), ("scaled", 1, k), scaled.at[0, k], scaled.at[1, k], peer(1))

    def spread(r, k, b):
        return nt_dot(scaled[r, k], foot_t[r, b * halo_w : (b + 1) * halo_w, :])

    def spread_all(r, b):
        return nt_dot(scaled[r].reshape(chan, obs), foot_t[r, b * halo_w : (b + 1) * halo_w, :])

    for b in range(4):
        total[b] = spread_all(0, b)
    for k in range(chunks):
        arrived(("scaled", 1, k), scaled.at[1, k], peer(1))
    for b in range(4):
        total[b] += spread_all(1, b)

    def last(k, b):
        here = total[b, k * rows : (k + 1) * rows, :]
        for dy in range(1, ny):
            here = here + spread(dy * CORES + 1, k, b)
        return here

    def send_rims(k):
        for dy in range(1, ny):
            arrived(("scaled", dy * CORES + 1, k), scaled.at[dy * CORES + 1, k], peer(1))
        rim_out[0, k] = last(k, 0).astype(BF16)
        rim_out[1, k] = last(k, 3).astype(BF16)
        send_sides("rim", k, rim_out, rim_in, lambda side: side, lambda side: 1 - side)

    for k in range(chunks):
        for dy in range(1, ny):
            r = dy * CORES
            arrived(("scaled", r, k), scaled.at[r, k], peer(r))
            send(("scaled", r + 1, k), ("scaled", r + 1, k), scaled.at[r, k], scaled.at[r + 1, k], peer(1))
        for dy in range(1, ny):
            for b in range(4):
                total[b, k * rows : (k + 1) * rows, :] += spread(dy * CORES, k, b)
        if k > 0:
            send_rims(k - 1)
    send_rims(chunks - 1)
    for b in (1, 2):
        for dy in range(1, ny):
            total[b] += spread_all(dy * CORES + 1, b)
    dep_ref[...] = dep_t[...].T
    for side in range(2):
        for k in range(chunks):
            arrived(("rim", k, side), rim_in.at[side, k], (turn, (left, right)[side]))
        rim = rim_in[side].reshape(chan, halo_w).astype(F32)
        sum_ref[side] = (total[1 + side] + rim).astype(BF16)
    for copy in started:
        copy.wait_send()


def finish_kernel(dep_ref, sum_ref, jac_ref, dep_hbm, adj_hbm, adj_ref, sems):
    dep_copy = pltpu.make_async_copy(dep_ref, dep_hbm, sems.at[0])
    dep_copy.start()
    jac = jac_ref[...]
    levels = jac.shape[0]
    halo_w = sum_ref.shape[2]
    for side in range(2):
        lanes = slice(side * halo_w, (side + 1) * halo_w)
        adj_ref[:, :, lanes] = nn_dot(jac, sum_ref[side]).reshape(levels, 1, halo_w)
    adj_copy = pltpu.make_async_copy(adj_ref, adj_hbm, sems.at[1])
    adj_copy.start()
    dep_copy.wait()
    adj_copy.wait()


def body(
    state, obs_start, foot_weight, obs_slot, obs_frac, live_count, obs_values, jacobian, inv_var
):
    n_tm = lax.axis_size("tm")
    n_space = lax.axis_size("space")
    ny = n_tm // CORES
    chunks = 2
    _, cols_dev, levels = state.shape
    obs, chan = obs_values.shape
    foot = foot_weight.shape[1]
    halo_w = cols_dev // 2
    width = cols_dev + 2 * halo_w
    rows = chan // chunks
    vmem = pl.BlockSpec(memory_space=pltpu.VMEM)
    live_space = pl.BlockSpec(memory_space=pltpu.SMEM)
    hbm = pl.BlockSpec(memory_space=pltpu.HBM)
    count = len(message_names(n_tm, chunks))
    departures, sums = pl.pallas_call(
        functools.partial(kernel, n_tm, n_space, chunks),
        name="departures_and_adjoint",
        out_shape=(
            pltpu.VMEM((obs, chan), F32),
            pltpu.VMEM((2, chan, halo_w), BF16),
        ),
        in_specs=[hbm] * 5 + [live_space] + [hbm] * 3,
        out_specs=(vmem, vmem),
        scratch_shapes=[
            pltpu.VMEM((levels, cols_dev), BF16),
            pltpu.VMEM((1, obs), jnp.int32),
            pltpu.VMEM((foot, obs), BF16),
            pltpu.VMEM((1, obs), jnp.int32),
            pltpu.VMEM((1, obs), F32),
            pltpu.VMEM((obs, chan), F32),
            pltpu.VMEM((levels, chan), BF16),
            pltpu.VMEM((1, chan), F32),
            pltpu.VMEM((4, chunks, rows, halo_w), BF16),
            pltpu.VMEM((n_tm, 2, obs), jnp.int32),
            pltpu.VMEM((n_tm, 2 * foot, obs), BF16),
            pltpu.VMEM((n_tm, width, obs), BF16),
            pltpu.VMEM((n_tm, chan, obs), F32),
            pltpu.VMEM((chan, obs), F32),
            pltpu.VMEM((chan, GROUP), F32),
            pltpu.VMEM((ny, chunks, rows, obs), BF16),
            pltpu.VMEM((ny, chunks, rows, obs), BF16),
            pltpu.VMEM((ny, chunks, rows, obs), BF16),
            pltpu.VMEM((ny, chunks, rows, obs), BF16),
            pltpu.VMEM((n_tm, chunks, rows, obs), BF16),
            pltpu.VMEM((4, chan, halo_w), F32),
            pltpu.VMEM((2, chunks, rows, halo_w), BF16),
            pltpu.VMEM((2, chunks, rows, halo_w), BF16),
            pltpu.VMEM((chan, obs), F32),
            pltpu.SemaphoreType.DMA((8,)),
            pltpu.SemaphoreType.DMA((count,)),
            pltpu.SemaphoreType.DMA((count,)),
        ],
        compiler_params=pltpu.CompilerParams(
            collective_id=0, has_side_effects=True, vmem_limit_bytes=58 * 1024 * 1024
        ),
    )(
        state[0].T,
        obs_start[None],
        foot_weight.T,
        obs_slot[None],
        obs_frac[None],
        live_count,
        obs_values,
        jacobian,
        inv_var[None],
    )
    departures, adjoint_t = pl.pallas_call(
        finish_kernel,
        name="write_outputs",
        out_shape=(
            jax.ShapeDtypeStruct((obs, chan), F32),
            jax.ShapeDtypeStruct((levels, 1, cols_dev), F32),
        ),
        in_specs=[vmem, vmem, vmem],
        out_specs=(hbm, hbm),
        scratch_shapes=[
            pltpu.VMEM((levels, 1, cols_dev), F32),
            pltpu.SemaphoreType.DMA((2,)),
        ],
        compiler_params=pltpu.CompilerParams(vmem_limit_bytes=4 * 1024 * 1024),
    )(departures, sums, jacobian)
    return (departures, adjoint_t.transpose(1, 2, 0))


def solution(mesh):
    return jax.shard_map(
        body,
        mesh=mesh,
        in_specs=(
            P("tm", "space", None),
            P(("tm", "space")),
            P(("tm", "space"), None),
            P(("tm", "space")),
            P(("tm", "space")),
            P("tm", "space"),
            P(("tm", "space"), None),
            P(),
            P(),
        ),
        out_specs=(P(("tm", "space"), None), P("tm", "space", None)),
        check_vma=False,
    )
```
